1024 devices in a mesh: fsdp: 64 (over x, y, core), tp: 16 (over z).
Axes of the slice: x: 4, y: 8, z: 16, core: 2. Of those that a mesh axis runs over, the one named last changes fastest.
Arguments:
- features: bfloat16 [8192, 8192], P('fsdp'), may hold values from -17 to 17
- key_partials: bfloat16 [8192, 16, 128], P('fsdp', 'tp'), may hold values from -0.109375 to 0.109375
- momentum: float32 [4096, 16, 128], P('fsdp', 'tp'), may hold values from -6 to 6
Outputs:
- update: float32 [4096, 16, 128], P('fsdp', 'tp')
- new_momentum: float32 [4096, 16, 128], P('fsdp', 'tp')
The draws below stay inside these ranges and needn't reach their ends.
All inputs are finite; a program needn't handle non-finite values.
Results may differ from the reference program's by a relative error of at most 0.0003.
Values may be sent and summed in bfloat16 or wider, within the bound.
A program may use at most 32 MiB of HBM per device.

```python
import math
import jax
import jax.numpy as jnp
from jax import lax

D_W = 8192
HD = 128
ITERS = 5
KVH = 8
TOKENS = 8192
N_FSDP = 64
N_TP = 16


def draw_features(key, part):
    first = jax.random.fold_in(jax.random.fold_in(key, 11), 0)
    columns = jnp.arange(D_W, dtype=jnp.float32) / D_W
    base = jnp.clip(jax.random.normal(first, (TOKENS, D_W), jnp.float32), -5.0, 5.0)
    scales = jnp.sqrt(1.0 + 2.0 * columns)
    return (base * scales[None, :]).astype(jnp.bfloat16)


def draw_key_partials(key, part):
    first = jax.random.fold_in(jax.random.fold_in(key, 23), 0)
    factor = (2.0 * TOKENS) ** (-0.5)
    values = jnp.clip(jax.random.normal(first, (TOKENS, N_TP, HD), jnp.float32), -4.0, 4.0) * factor
    return values.astype(jnp.bfloat16)


def levels(rng, dims, shards, least, largest):
    gain, own = 1.0, jax.random.fold_in(rng, 6)
    for axis_at, blocks in shards:
        heights = jnp.exp(jax.random.uniform(jax.random.fold_in(own, axis_at), (blocks,), jnp.float32, least / len(shards), largest / len(shards)))
        gain = gain * jnp.repeat(heights, dims[axis_at] // blocks).reshape([-1 if axis == axis_at else 1 for axis in range(len(dims))])
    return gain


def noise(rng, extent, scale, most, shards=(), held_as=jnp.bfloat16):
    entries = scale * jax.random.normal(rng, extent, jnp.float32)
    if shards:
        entries = entries * levels(rng, extent, shards, -0.22, 0.18)
    return jnp.clip(entries, -most, most).astype(held_as)


def setup_inputs(seed: int = 0) -> dict:
    key_of = jax.random.split(jax.random.key(seed), 4)
    features = draw_features(jax.random.fold_in(key_of[3], 71), 0)
    key_partials = draw_key_partials(jax.random.fold_in(key_of[3], 71), 0)
    momentum = noise(key_of[2], (D_W // 2, N_TP, HD), 1.0, 6.0, ((0, 64), (1, 16)), jnp.float32)
    return {"features": features, "key_partials": key_partials, "momentum": momentum}


retain = 0.95
first_coef = 3.4445
second_coef = -4.775
third_coef = 2.0315
epsilon = 1e-07
shrink = 0.2

def dense_layout(stored):
    halves = D_W // (2 * N_FSDP)
    return stored.reshape(N_FSDP, halves, KVH, 2, HD).transpose(2, 0, 3, 1, 4).reshape(KVH, D_W, HD)

def stored_layout(dense):
    halves = D_W // (2 * N_FSDP)
    return dense.reshape(KVH, N_FSDP, 2, halves, HD).transpose(1, 3, 0, 2, 4).reshape(N_FSDP * halves, KVH * 2, HD)

def reference(features, key_partials, momentum):
    precise = lax.Precision.HIGHEST
    widened = features.astype(jnp.float32)
    summed = key_partials.astype(jnp.float32).reshape(TOKENS, KVH, 2, HD).sum(axis=2).reshape(TOKENS, KVH * HD)
    grads = lax.dot_general(widened, summed, (((0,), (0,)), ((), ())), precision=precise)
    grads = grads.reshape(D_W, KVH, HD).transpose(1, 0, 2)
    moment = dense_layout(momentum)
    fresh = retain * moment + grads
    blend = grads + retain * fresh
    length = jnp.sqrt(lax.optimization_barrier(jnp.sum(blend * blend, axis=(1, 2), keepdims=True)))
    state = blend / (length + epsilon)
    for step in range(ITERS):
        gram = jnp.einsum('hrd,hre->hde', state, state, precision=precise)
        square = jnp.einsum('hde,hef->hdf', gram, gram, precision=precise)
        poly = second_coef * gram + third_coef * square
        state = first_coef * state + jnp.einsum('hrd,hde->hre', state, poly, precision=precise)
    update = shrink * math.sqrt(D_W) * state
    return (stored_layout(update), stored_layout(fresh))
```

```python
import math

import jax
import jax.numpy as jnp
from jax import lax
from jax.experimental import pallas as pl
from jax.experimental.pallas import tpu as pltpu
from jax.sharding import PartitionSpec as P

D_W = 8192
ITERS = 5
NX = 4
HD = 128
HALF = 64

retain = 0.95
first_coef = 3.4445
second_coef = -4.775
third_coef = 2.0315
epsilon = 1e-07
shrink = 0.2

MESH = pl.DeviceIdType.MESH
PRECISE = lax.Precision.HIGHEST


def chunk_order(chunks):
    return {1: (0,), 2: (1, 0), 4: (2, 1, 3, 0)}[chunks]


def step_kernel(
    ny, feat, keys, mom, upd, fresh_out,
    fv, fr, kv, lhs, mv, xs1, xr1, xk, xs2, xr2, ys, yr, gs, gr, hr, ag,
    load_sem, key_send, key_recv, f_send, f_recv, s1_send, s1_recv, s0_send, s0_recv,
    x2_send, x2_recv, y_send, y_recv, ga_send, ga_recv, gb_send, gb_recv, gc_send, gc_recv,
):
    chunks = ny // 2
    order = chunk_order(chunks)
    me = lax.axis_index("fsdp")
    z = lax.axis_index("tp")
    core = lax.rem(me, 2)
    chip = lax.div(me, 2)
    y = lax.rem(chip, ny)
    x = lax.div(chip, ny)
    par = lax.rem(z, 2)
    ky = lax.div(y, 2)
    zpair = z - par

    def device(xx, yy, cc, pp):
        return ((xx * ny + yy) * 2 + cc, zpair + pp)

    member = (x * 2 + core) * 2 + par

    def member_device(b):
        return device(lax.div(b, 4), y, lax.rem(lax.div(b, 2), 2), lax.rem(b, 2))

    barrier = pltpu.get_barrier_semaphore()

    def greet_member(d, carry):
        pl.semaphore_signal(
            barrier, inc=1, device_id=member_device(lax.rem(member + d, 16)), device_id_type=MESH
        )
        return carry

    def greet_column(d, carry):
        pl.semaphore_signal(
            barrier, inc=1, device_id=device(x, lax.rem(y + d, ny), core, par), device_id_type=MESH
        )
        return carry

    lax.fori_loop(1, ny, greet_column, 0)
    lax.fori_loop(1, 16, greet_member, 0)

    key_load = pltpu.make_async_copy(keys, kv.at[0, 0], load_sem.at[2])
    key_load.start()
    mom_load = pltpu.make_async_copy(mom, mv, load_sem.at[3])
    mom_load.start()

    def load_tiles(q, owner_core):
        def body(t, carry):
            k = lax.div(t, 8)
            r = lax.rem(t, 8)
            xx = lax.div(r, 2)
            j = lax.rem(r, 2)
            col = ((xx * ny + 2 * k + j) * 2 + owner_core) * HD
            pltpu.make_async_copy(
                feat.at[:, pl.ds(pl.multiple_of(col, HD), HD)], fv.at[q, k, r], load_sem.at[q]
            ).start()
            return carry

        lax.fori_loop(0, 8 * chunks, body, 0)

    load_tiles(1, 1 - core)
    load_tiles(0, core)
    key_load.wait()
    pltpu.make_async_copy(fv.at[1], fv.at[1], load_sem.at[1]).wait()

    pl.semaphore_wait(barrier, 15 + ny - 1)

    key_copies = []
    for n, (cc, pp, slot) in enumerate(
        (
            (1 - core, 1 - par, (1, 1)),
            (core, 1 - par, (1, 0)),
            (1 - core, par, (0, 1)),
        )
    ):
        copy = pltpu.make_async_remote_copy(
            src_ref=kv.at[0, 0],
            dst_ref=kv.at[slot[0], slot[1]],
            send_sem=key_send.at[n],
            recv_sem=key_recv.at[n],
            device_id=device(x, y, cc, pp),
            device_id_type=MESH,
        )
        copy.start()
        key_copies.append(copy)
    f_copies = []
    for i in range(chunks):
        k = lax.rem(ky + order[i], chunks)
        copy = pltpu.make_async_remote_copy(
            src_ref=fv.at[1, k],
            dst_ref=fr.at[k],
            send_sem=f_send.at[i],
            recv_sem=f_recv.at[i],
            device_id=device(x, y, 1 - core, par),
            device_id_type=MESH,
        )
        copy.start()
        f_copies.append(copy)

    pltpu.make_async_copy(fv.at[0], fv.at[0], load_sem.at[0]).wait()
    for copy in key_copies:
        copy.wait_recv()
    for r in range(2):
        for f in range(2):
            lhs[r * HD : (r + 1) * HD, f * HD : (f + 1) * HD] = kv[r, f].T

    lane = lax.broadcasted_iota(jnp.int32, (HD, HD), 1)
    kept = jnp.logical_and(lane >= HALF * par, lane < HALF * par + HALF)

    def partial_for(k, dest):
        top = jnp.concatenate([fv[0, k, 2 * dest], fv[0, k, 2 * dest + 1]], axis=1)
        bottom = jnp.concatenate([fr[k, 2 * dest], fr[k, 2 * dest + 1]], axis=1)
        rhs = jnp.concatenate([top, bottom], axis=0)
        both = jnp.dot(lhs[...], rhs, preferred_element_type=jnp.float32)
        both = both[:HD] + both[HD:]
        low, high = both[:, :HD], both[:, HD:]
        still = jnp.where(par == 0, low, high)
        moved = jnp.where(par == 0, high, low)
        return jnp.where(kept, still, pltpu.roll(moved, HALF, axis=1))

    near = (x + 1 - 2 * lax.rem(x, 2), 3 - x)
    across = lax.rem(x + 2, NX)

    def first(i):
        return near[i % 2]

    def second(i):
        return near[1 - i % 2]

    def chunk(i):
        return lax.rem(ky + order[i], chunks)

    def send(src, dst, send_sem, recv_sem, target):
        copy = pltpu.make_async_remote_copy(
            src_ref=src,
            dst_ref=dst,
            send_sem=send_sem,
            recv_sem=recv_sem,
            device_id=target,
            device_id_type=MESH,
        )
        copy.start()
        return copy

    s1, s0, x2, ysends = {}, {}, {}, []

    def send_far(i):
        s1[i] = send(
            xs1.at[i, 1], xr1.at[i, 1], s1_send.at[i], s1_recv.at[i], device(first(i), y, core, par)
        )

    def send_near(i):
        s0[i] = send(
            xs1.at[i, 0], xr1.at[i, 0], s0_send.at[i], s0_recv.at[i], device(first(i), y, core, par)
        )

    def forward(i):
        s1[i].wait_recv()
        xs2[i] = xk[i, 0] + xr1[i, 1]
        x2[i] = send(xs2.at[i], xr2.at[i], x2_send.at[i], x2_recv.at[i], device(second(i), y, core, par))

    def finish(i):
        s0[i].wait_recv()
        x2[i].wait_recv()
        ys[i] = (xk[i, 1] + xr1[i, 0] + xr2[i]).T
        k = chunk(i)
        if order[i] == 0:
            j = 1 - lax.rem(y, 2)
            targets = [(2 * ky + j, j)]
        else:
            targets = [(2 * k, 0), (2 * k + 1, 1)]
        for yy, j in targets:
            ysends.append(
                send(
                    ys.at[i, pl.ds(pl.multiple_of(j * HALF, HALF), HALF)],
                    yr.at[y],
                    y_send.at[len(ysends)],
                    y_recv.at[y],
                    device(x, yy, core, par),
                )
            )

    lead = list(range(min(2, chunks)))
    rest = list(range(len(lead), chunks))
    for i in lead:
        f_copies[i].wait_recv()
        xs1[i, 1] = partial_for(chunk(i), across)
        send_far(i)
    for i in lead:
        xs1[i, 0] = partial_for(chunk(i), first(i))
        send_near(i)
    for i in rest:
        f_copies[i].wait_recv()
        xs1[i, 1] = partial_for(chunk(i), across)
        send_far(i)
    for i in lead:
        xk[i, 0] = partial_for(chunk(i), second(i))
    for i in rest:
        xs1[i, 0] = partial_for(chunk(i), first(i))
    for i in lead:
        forward(i)
    for i in rest:
        send_near(i)
    for i in rest:
        xk[i, 0] = partial_for(chunk(i), second(i))
    for i in lead + rest:
        xk[i, 1] = partial_for(chunk(i), x)
    for i in rest:
        forward(i)
    for i in lead + rest:
        finish(i)

    mom_load.wait()
    last = len(order) - 1
    grads = ys[last, pl.ds(pl.multiple_of(lax.rem(y, 2) * HALF, HALF), HALF), :]
    for d in range(1, ny):
        yy = lax.rem(y + d, ny)
        pltpu.make_async_remote_copy(
            src_ref=yr.at[yy],
            dst_ref=yr.at[yy],
            send_sem=y_send.at[0],
            recv_sem=y_recv.at[yy],
            device_id=device(x, yy, core, par),
            device_id_type=MESH,
        ).wait_recv()
        grads = grads + yr[yy]

    fresh = retain * mv[...] + grads
    fresh_out[...] = fresh
    blend = grads + retain * fresh
    contract = (((0,), (0,)), ((), ()))
    gs[...] = lax.dot_general(
        blend, blend, contract, precision=PRECISE, preferred_element_type=jnp.float32
    )

    def piece(b):
        return pl.ds(pl.multiple_of(b * 8, 8), 8)

    def scatter(d, carry):
        b = lax.rem(member + d, 16)
        pltpu.make_async_remote_copy(
            src_ref=gs.at[piece(b)],
            dst_ref=gr.at[member],
            send_sem=ga_send.at[b],
            recv_sem=ga_recv.at[member],
            device_id=member_device(b),
            device_id_type=MESH,
        ).start()
        return carry

    lax.fori_loop(1, 16, scatter, 0)
    gr[member] = gs[piece(member), :]

    def scatter_wait(d, carry):
        b = lax.rem(member + d, 16)
        copy = pltpu.make_async_remote_copy(
            src_ref=gs.at[piece(b)],
            dst_ref=gr.at[b],
            send_sem=ga_send.at[b],
            recv_sem=ga_recv.at[b],
            device_id=member_device(b),
            device_id_type=MESH,
        )
        copy.wait_recv()
        return carry

    lax.fori_loop(1, 16, scatter_wait, 0)
    hr[y] = jnp.sum(gr[...], axis=0)

    def column(d, carry):
        yy = lax.rem(y + d, ny)
        pltpu.make_async_remote_copy(
            src_ref=hr.at[y],
            dst_ref=hr.at[y],
            send_sem=gb_send.at[yy],
            recv_sem=gb_recv.at[y],
            device_id=device(x, yy, core, par),
            device_id_type=MESH,
        ).start()
        return carry

    lax.fori_loop(1, ny, column, 0)

    def column_wait(d, carry):
        yy = lax.rem(y + d, ny)
        pltpu.make_async_remote_copy(
            src_ref=hr.at[y],
            dst_ref=hr.at[yy],
            send_sem=gb_send.at[yy],
            recv_sem=gb_recv.at[yy],
            device_id=device(x, yy, core, par),
            device_id_type=MESH,
        ).wait_recv()
        return carry

    lax.fori_loop(1, ny, column_wait, 0)
    ag[member] = jnp.sum(hr[...], axis=0)

    def gather(d, carry):
        b = lax.rem(member + d, 16)
        pltpu.make_async_remote_copy(
            src_ref=ag.at[member],
            dst_ref=ag.at[member],
            send_sem=gc_send.at[b],
            recv_sem=gc_recv.at[member],
            device_id=member_device(b),
            device_id_type=MESH,
        ).start()
        return carry

    lax.fori_loop(1, 16, gather, 0)

    def gather_wait(d, carry):
        b = lax.rem(member + d, 16)
        pltpu.make_async_remote_copy(
            src_ref=ag.at[member],
            dst_ref=ag.at[b],
            send_sem=gc_send.at[b],
            recv_sem=gc_recv.at[b],
            device_id=member_device(b),
            device_id_type=MESH,
        ).wait_recv()
        return carry

    lax.fori_loop(1, 16, gather_wait, 0)

    gram = ag[...].reshape(HD, HD)
    row = lax.broadcasted_iota(jnp.int32, (HD, HD), 0)
    identity = jnp.where(row == lane, 1.0, 0.0).astype(jnp.float32)
    total = jnp.sum(gram * identity, axis=(0, 1), keepdims=True)
    inverse = 1.0 / (jnp.sqrt(total) + epsilon)

    def dot(a, b):
        return jnp.dot(a, b, precision=PRECISE, preferred_element_type=jnp.float32)

    state = blend * inverse
    gram = gram * (inverse * inverse)
    for step in range(ITERS):
        square = dot(gram, gram)
        poly = first_coef * identity + second_coef * gram + third_coef * square
        state = dot(state, poly)
        if step < ITERS - 1:
            gram = dot(dot(gram, poly), poly)
    upd[...] = shrink * math.sqrt(D_W) * state

    for copy in key_copies + f_copies + ysends:
        copy.wait_send()
    for group in (s1, s0, x2):
        for copy in group.values():
            copy.wait_send()

    def drain_members(d, carry):
        b = lax.rem(member + d, 16)
        for src, sem in ((gs.at[piece(b)], ga_send), (ag.at[member], gc_send)):
            pltpu.make_async_remote_copy(
                src_ref=src,
                dst_ref=gr.at[member],
                send_sem=sem.at[b],
                recv_sem=ga_recv.at[member],
                device_id=member_device(b),
                device_id_type=MESH,
            ).wait_send()
        return carry

    lax.fori_loop(1, 16, drain_members, 0)

    def drain_column(d, carry):
        yy = lax.rem(y + d, ny)
        pltpu.make_async_remote_copy(
            src_ref=hr.at[y],
            dst_ref=hr.at[y],
            send_sem=gb_send.at[yy],
            recv_sem=gb_recv.at[y],
            device_id=device(x, yy, core, par),
            device_id_type=MESH,
        ).wait_send()
        return carry

    lax.fori_loop(1, ny, drain_column, 0)


def on_device(features, key_partials, momentum):
    ny = lax.axis_size("fsdp") // (2 * NX)
    chunks = ny // 2
    f32, bf16 = jnp.float32, jnp.bfloat16
    dma = pltpu.SemaphoreType.DMA
    block = jax.ShapeDtypeStruct((HALF, HD), f32)
    anywhere = pl.BlockSpec(memory_space=pl.ANY)
    vmem = pl.BlockSpec(memory_space=pltpu.VMEM)

    def body(*refs):
        step_kernel(ny, *refs)

    update, fresh = pl.pallas_call(
        body,
        name="muon_step",
        out_shape=(block, block),
        in_specs=[anywhere] * 3,
        out_specs=(vmem, vmem),
        scratch_shapes=[
            pltpu.VMEM((2, chunks, 8, HD, HD), bf16),
            pltpu.VMEM((chunks, 8, HD, HD), bf16),
            pltpu.VMEM((2, 2, HD, HD), bf16),
            pltpu.VMEM((2 * HD, 2 * HD), bf16),
            pltpu.VMEM((HALF, HD), f32),
            pltpu.VMEM((chunks, 2, HD, HD), f32),
            pltpu.VMEM((chunks, 2, HD, HD), f32),
            pltpu.VMEM((chunks, 2, HD, HD), f32),
            pltpu.VMEM((chunks, HD, HD), f32),
            pltpu.VMEM((chunks, HD, HD), f32),
            pltpu.VMEM((chunks, HD, HD), f32),
            pltpu.VMEM((ny, HALF, HD), f32),
            pltpu.VMEM((HD, HD), f32),
            pltpu.VMEM((16, 8, HD), f32),
            pltpu.VMEM((ny, 8, HD), f32),
            pltpu.VMEM((16, 8, HD), f32),
            dma((4,)),
            dma((3,)), dma((3,)),
            dma((chunks,)), dma((chunks,)),
            dma((chunks,)), dma((chunks,)),
            dma((chunks,)), dma((chunks,)),
            dma((chunks,)), dma((chunks,)),
            dma((ny,)), dma((ny,)),
            dma((16,)), dma((16,)),
            dma((ny,)), dma((ny,)),
            dma((16,)), dma((16,)),
        ],
        compiler_params=pltpu.CompilerParams(collective_id=0, has_side_effects=True),
    )(features, key_partials[:, 0, :], momentum[:, 0, :])
    return (update[:, None, :], fresh[:, None, :])


def solution(mesh):
    placed = (P("fsdp", None), P("fsdp", "tp", None), P("fsdp", "tp", None))
    return jax.shard_map(
        on_device,
        mesh=mesh,
        in_specs=placed,
        out_specs=(P("fsdp", "tp", None), P("fsdp", "tp", None)),
        check_vma=False,
    )
```

```python
import math

import jax
import jax.numpy as jnp
from jax import lax
from jax.experimental import pallas as pl
from jax.experimental.pallas import tpu as pltpu
from jax.sharding import PartitionSpec as P

D_W = 8192
ITERS = 5
NX = 4
HD = 128
HALF = 64

retain = 0.95
first_coef = 3.4445
second_coef = -4.775
third_coef = 2.0315
epsilon = 1e-07
shrink = 0.2

MESH = pl.DeviceIdType.MESH
PRECISE = lax.Precision.HIGHEST


def chunk_order(chunks):
    return {1: (0,), 2: (1, 0), 4: (2, 1, 3, 0)}[chunks]


def step_kernel(
    ny, feat, keys, mom, state_out, grads_out,
    fv, fr, kv, lhs, mv, sf, pn, px, rx, fw, ys, yr, gs, gr, hr, ag,
    load_sem, key_sem, f_send, f_recv, x_send, x_recv, y_send, y_recv, g_send, g_recv,
):
    chunks = ny // 2
    order = chunk_order(chunks)
    me = lax.axis_index("fsdp")
    z = lax.axis_index("tp")
    core = lax.rem(me, 2)
    chip = lax.div(me, 2)
    y = lax.rem(chip, ny)
    x = lax.div(chip, ny)
    par = lax.rem(z, 2)
    ky = lax.div(y, 2)
    zpair = z - par

    xs = [x] + [lax.rem(x + d, NX) for d in range(1, NX)]
    yy = [y] + [lax.rem(y + d, ny) for d in range(1, ny)]
    cs = (core, 1 - core)
    ps = (par, 1 - par)

    def device(xx, yv, cc, pp):
        return ((xx * ny + yv) * 2 + cc, zpair + pp)

    def number(xx, cc, pp):
        return (xx * 2 + cc) * 2 + pp

    member = number(x, core, par)
    others = [
        (xs[dx], cs[dc], ps[dp])
        for dx in (2, 1, 3, 0)
        for dp in (1, 0)
        for dc in (1, 0)
        if (dx, dp, dc) != (0, 0, 0)
    ]
    far_first = sorted(range(1, ny), key=lambda d: -min(d, ny - d))

    def start(src, dst, send_sem, recv_sem, target):
        pltpu.make_async_remote_copy(
            src_ref=src,
            dst_ref=dst,
            send_sem=send_sem,
            recv_sem=recv_sem,
            device_id=target,
            device_id_type=MESH,
        ).start()

    def await_bytes(ref, sem):
        pltpu.make_async_copy(ref, ref, sem).wait()

    key_load = pltpu.make_async_copy(keys, kv.at[0], load_sem.at[chunks])
    key_load.start()
    barrier = pltpu.get_barrier_semaphore()
    for d in far_first:
        pl.semaphore_signal(
            barrier, inc=1, device_id=device(x, yy[d], core, par), device_id_type=MESH
        )
    for xx, cc, pp in others:
        pl.semaphore_signal(barrier, inc=1, device_id=device(xx, y, cc, pp), device_id_type=MESH)

    def chunk(i):
        return lax.rem(ky + order[i], chunks)

    ks = [chunk(i) for i in range(chunks)]

    wide = 4 * HD
    for i in range(chunks):
        for xx in range(NX):
            col = pl.multiple_of((xx * ny + 2 * ks[i]) * 2 * HD, wide)
            pltpu.make_async_copy(
                feat.at[:, pl.ds(col, wide)], fv.at[ks[i], xx], load_sem.at[i]
            ).start()
    mom_load = pltpu.make_async_copy(mom, mv, load_sem.at[chunks + 1])
    mom_load.start()

    key_load.wait()
    pl.semaphore_wait(barrier, 15 + ny - 1)

    for cc, pp, slot in ((cs[1], ps[1], 3), (core, ps[1], 2), (cs[1], par, 1)):
        start(kv.at[0], kv.at[slot], key_sem.at[0], key_sem.at[1], device(x, y, cc, pp))
    for i in range(chunks):
        await_bytes(fv.at[ks[i]], load_sem.at[i])
        for xx in (2, 1, 3, 0):
            for j in range(2):
                col = pl.multiple_of((2 * j + 1 - core) * HD, HD)
                start(
                    fv.at[ks[i], xs[xx], :, pl.ds(col, HD)],
                    fr.at[ks[i], xs[xx], :, pl.ds(j * HD, HD)],
                    f_send.at[0],
                    f_recv.at[i],
                    device(x, y, 1 - core, par),
                )

    await_bytes(kv.at[pl.ds(1, 3)], key_sem.at[1])
    for r in range(2):
        for f in range(2):
            lhs[r * HD : (r + 1) * HD, f * HD : (f + 1) * HD] = kv[2 * r + f].T

    lane = lax.broadcasted_iota(jnp.int32, (HD, HD), 1)
    kept = jnp.logical_and(lane >= HALF * par, lane < HALF * par + HALF)
    first_tile = pl.ds(pl.multiple_of(core * HD, HD), HD)
    second_tile = pl.ds(pl.multiple_of((2 + core) * HD, HD), HD)

    def partial_for(k, dest):
        top = jnp.concatenate([fv[k, dest, :, first_tile], fv[k, dest, :, second_tile]], axis=1)
        rhs = jnp.concatenate([top, fr[k, dest]], axis=0)
        both = jnp.dot(lhs[...], rhs, preferred_element_type=jnp.float32)
        both = both[:HD] + both[HD:]
        low, high = both[:, :HD], both[:, HD:]
        still = jnp.where(par == 0, low, high)
        moved = jnp.where(par == 0, high, low)
        return jnp.where(kept, still, pltpu.roll(moved, HALF, axis=1))

    near = (x + 1 - 2 * lax.rem(x, 2), 3 - x)
    halves = (pl.ds(0, HALF), pl.ds(HALF, HALF))

    def step_one(i):
        await_bytes(fr.at[ks[i]], f_recv.at[i])
        sf[i] = partial_for(ks[i], xs[2])
        for h in range(2):
            start(
                sf.at[i, halves[h]], rx.at[0, i, h], x_send.at[0], x_recv.at[0, i, h],
                device(near[h], y, core, par),
            )
        for a in range(2):
            pn[i, a] = partial_for(ks[i], near[a])
        for h in range(2):
            start(
                pn.at[i, h, halves[h]], rx.at[1, i, h], x_send.at[0], x_recv.at[1, i, h],
                device(near[h], y, core, par),
            )

    def step_two(i):
        for h in range(2):
            await_bytes(rx.at[0, i, h], x_recv.at[0, i, h])
            fw[i, h] = pn[i, 1 - h, halves[h], :] + rx[0, i, h]
            start(
                fw.at[i, h], rx.at[2, i, h], x_send.at[0], x_recv.at[2, i, h],
                device(near[1 - h], y, core, par),
            )

    def own(i):
        px[i] = partial_for(ks[i], x)

    def finish(i):
        for stage in (1, 2):
            for h in range(2):
                await_bytes(rx.at[stage, i, h], x_recv.at[stage, i, h])
        total = px[i] + (rx[1, i] + rx[2, i]).reshape(HD, HD)
        ys[i] = total.T
        if order[i] == 0:
            j = 1 - lax.rem(y, 2)
            targets = [(2 * ky + j, j)]
        else:
            targets = [(2 * ks[i], 0), (2 * ks[i] + 1, 1)]
        for yv, j in targets:
            rows = pl.ds(pl.multiple_of(j * HALF, HALF), HALF)
            start(ys.at[i, rows], yr.at[y], y_send.at[0], y_recv.at[y], device(x, yv, core, par))

    if chunks == 4:
        step_one(0)
        step_one(1)
        step_two(0)
        step_one(2)
        step_two(1)
        step_one(3)
        for i in range(chunks):
            own(i)
        finish(0)
        step_two(2)
        finish(1)
        step_two(3)
        finish(2)
        finish(3)
    else:
        for i in range(chunks):
            step_one(i)
        for i in range(chunks):
            step_two(i)
            own(i)
        for i in range(chunks):
            finish(i)

    mom_load.wait()
    grads = ys[chunks - 1, pl.ds(pl.multiple_of(lax.rem(y, 2) * HALF, HALF), HALF), :]
    for d in far_first:
        await_bytes(yr.at[yy[d]], y_recv.at[yy[d]])
        grads = grads + yr[yy[d]]

    grads_out[...] = grads
    blend = grads + retain * (retain * mv[...] + grads)
    contract = (((0,), (0,)), ((), ()))
    gs[...] = lax.dot_general(
        blend, blend, contract, precision=PRECISE, preferred_element_type=jnp.float32
    )

    def piece(b):
        return pl.ds(pl.multiple_of(b * 8, 8), 8)

    for xx, cc, pp in others:
        start(
            gs.at[piece(number(xx, cc, pp))], gr.at[member], g_send.at[0], g_recv.at[0],
            device(xx, y, cc, pp),
        )
    gr[member] = gs[piece(member), :]
    await_bytes(gr.at[pl.ds(0, 15)], g_recv.at[0])
    hr[y] = jnp.sum(gr[...], axis=0)
    for d in far_first:
        start(hr.at[y], hr.at[y], g_send.at[1], g_recv.at[1], device(x, yy[d], core, par))
    await_bytes(hr.at[pl.ds(0, ny - 1)], g_recv.at[1])
    ag[member] = jnp.sum(hr[...], axis=0)
    for xx, cc, pp in others:
        start(
            ag.at[member], ag.at[member], g_send.at[2], g_recv.at[2], device(xx, y, cc, pp)
        )
    await_bytes(ag.at[pl.ds(0, 15)], g_recv.at[2])

    gram = ag[...].reshape(HD, HD)
    row = lax.broadcasted_iota(jnp.int32, (HD, HD), 0)
    identity = jnp.where(row == lane, 1.0, 0.0).astype(jnp.float32)
    total = jnp.sum(gram * identity, axis=(0, 1), keepdims=True)
    inverse = 1.0 / (jnp.sqrt(total) + epsilon)

    def dot(a, b):
        return jnp.dot(a, b, precision=PRECISE, preferred_element_type=jnp.float32)

    state = blend * inverse
    gram = gram * (inverse * inverse)
    for step in range(ITERS):
        square = dot(gram, gram)
        poly = first_coef * identity + second_coef * gram + third_coef * square
        state = dot(state, poly)
        if step < ITERS - 1:
            gram = dot(dot(gram, poly), poly)
    state_out[...] = state

    await_bytes(kv.at[pl.ds(1, 3)], key_sem.at[0])
    await_bytes(fr, f_send.at[0])
    await_bytes(rx, x_send.at[0])
    await_bytes(yr.at[pl.ds(0, ny - 1)], y_send.at[0])
    await_bytes(gr.at[pl.ds(0, 15)], g_send.at[0])
    await_bytes(hr.at[pl.ds(0, ny - 1)], g_send.at[1])
    await_bytes(ag.at[pl.ds(0, 15)], g_send.at[2])


def on_device(features, key_partials, momentum):
    ny = lax.axis_size("fsdp") // (2 * NX)
    chunks = ny // 2
    f32, bf16 = jnp.float32, jnp.bfloat16
    dma = pltpu.SemaphoreType.DMA
    block = jax.ShapeDtypeStruct((HALF, HD), f32)
    hbm = pl.BlockSpec(memory_space=pltpu.HBM)
    vmem = pl.BlockSpec(memory_space=pltpu.VMEM)
    moment = momentum[:, 0, :]

    def body(*refs):
        step_kernel(ny, *refs)

    state, grads = pl.pallas_call(
        body,
        name="muon_step",
        out_shape=(block, block),
        in_specs=[hbm] * 3,
        out_specs=(vmem, vmem),
        scratch_shapes=[
            pltpu.VMEM((chunks, NX, HD, 4 * HD), bf16),
            pltpu.VMEM((chunks, NX, HD, 2 * HD), bf16),
            pltpu.VMEM((4, HD, HD), bf16),
            pltpu.VMEM((2 * HD, 2 * HD), bf16),
            pltpu.VMEM((HALF, HD), f32),
            pltpu.VMEM((chunks, HD, HD), f32),
            pltpu.VMEM((chunks, 2, HD, HD), f32),
            pltpu.VMEM((chunks, HD, HD), f32),
            pltpu.VMEM((3, chunks, 2, HALF, HD), f32),
            pltpu.VMEM((chunks, 2, HALF, HD), f32),
            pltpu.VMEM((chunks, HD, HD), f32),
            pltpu.VMEM((ny, HALF, HD), f32),
            pltpu.VMEM((HD, HD), f32),
            pltpu.VMEM((16, 8, HD), f32),
            pltpu.VMEM((ny, 8, HD), f32),
            pltpu.VMEM((16, 8, HD), f32),
            dma((chunks + 2,)),
            dma((2,)),
            dma((1,)), dma((chunks,)),
            dma((1,)), dma((3, chunks, 2)),
            dma((1,)), dma((ny,)),
            dma((3,)), dma((3,)),
        ],
        compiler_params=pltpu.CompilerParams(
            collective_id=0, has_side_effects=True, vmem_limit_bytes=16 * 1024 * 1024
        ),
    )(*(pltpu.with_memory_space_constraint(v, pltpu.HBM) for v in (features, key_partials[:, 0, :], moment)))
    update = shrink * math.sqrt(D_W) * state
    return (update[:, None, :], (retain * moment + grads)[:, None, :])


def solution(mesh):
    placed = (P("fsdp", None), P("fsdp", "tp", None), P("fsdp", "tp", None))
    return jax.shard_map(
        on_device,
        mesh=mesh,
        in_specs=placed,
        out_specs=(P("fsdp", "tp", None), P("fsdp", "tp", None)),
        check_vma=False,
    )
```

```python
import math

import jax
import jax.numpy as jnp
from jax import lax
from jax.experimental import pallas as pl
from jax.experimental.pallas import tpu as pltpu
from jax.sharding import PartitionSpec as P

D_W = 8192
ITERS = 5
NX = 4
HD = 128
HALF = 64

retain = 0.95
first_coef = 3.4445
second_coef = -4.775
third_coef = 2.0315
epsilon = 1e-07
shrink = 0.2

MESH = pl.DeviceIdType.MESH
PRECISE = lax.Precision.HIGHEST


def chunk_order(chunks):
    return {1: (0,), 2: (1, 0), 4: (2, 1, 3, 0)}[chunks]


def step_kernel(
    ny, feat, keys, mom, state_out, grads_out,
    fv, fr, kv, lhs, mv, sf, pn, px, rx, fw, ys, yr, sy, ry, sk, qs, xd, gs, gr, hr, ag,
    load_sem, key_sem, f_send, f_recv, x_send, x_recv, y_send, y_recv, p_send, p_recv, d_send, d_recv,
    g_send, g_recv,
):
    chunks = ny // 2
    order = chunk_order(chunks)
    me = lax.axis_index("fsdp")
    z = lax.axis_index("tp")
    core = lax.rem(me, 2)
    chip = lax.div(me, 2)
    y = lax.rem(chip, ny)
    x = lax.div(chip, ny)
    par = lax.rem(z, 2)
    ky = lax.div(y, 2)
    zpair = z - par

    xs = [x] + [lax.rem(x + d, NX) for d in range(1, NX)]
    yy = [y] + [lax.rem(y + d, ny) for d in range(1, ny)]
    cs = (core, 1 - core)
    ps = (par, 1 - par)

    def device(xx, yv, cc, pp):
        return ((xx * ny + yv) * 2 + cc, zpair + pp)

    def number(xx, cc, pp):
        return (xx * 2 + cc) * 2 + pp

    member = number(x, core, par)
    others = [
        (xs[dx], cs[dc], ps[dp])
        for dx in (2, 1, 3, 0)
        for dp in (1, 0)
        for dc in (1, 0)
        if (dx, dp, dc) != (0, 0, 0)
    ]
    far_first = sorted(range(1, ny), key=lambda d: -min(d, ny - d))

    def start(src, dst, send_sem, recv_sem, target):
        pltpu.make_async_remote_copy(
            src_ref=src,
            dst_ref=dst,
            send_sem=send_sem,
            recv_sem=recv_sem,
            device_id=target,
            device_id_type=MESH,
        ).start()

    def await_bytes(ref, sem):
        pltpu.make_async_copy(ref, ref, sem).wait()

    key_load = pltpu.make_async_copy(keys, kv.at[0], load_sem.at[chunks])
    key_load.start()
    barrier = pltpu.get_barrier_semaphore()
    for d in far_first:
        pl.semaphore_signal(
            barrier, inc=1, device_id=device(x, yy[d], core, par), device_id_type=MESH
        )
    for xx, cc, pp in others:
        pl.semaphore_signal(barrier, inc=1, device_id=device(xx, y, cc, pp), device_id_type=MESH)

    def chunk(i):
        return lax.rem(ky + order[i], chunks)

    ks = [chunk(i) for i in range(chunks)]

    wide = 4 * HD
    for i in range(chunks):
        for xx in range(NX):
            col = pl.multiple_of((xx * ny + 2 * ks[i]) * 2 * HD, wide)
            pltpu.make_async_copy(
                feat.at[:, pl.ds(col, wide)], fv.at[ks[i], xx], load_sem.at[i]
            ).start()
    mom_load = pltpu.make_async_copy(mom, mv, load_sem.at[chunks + 1])
    mom_load.start()

    key_load.wait()
    pl.semaphore_wait(barrier, 15 + ny - 1)

    for cc, pp, slot in ((cs[1], ps[1], 3), (core, ps[1], 2), (cs[1], par, 1)):
        start(kv.at[0], kv.at[slot], key_sem.at[0], key_sem.at[1], device(x, y, cc, pp))
    for i in range(chunks):
        await_bytes(fv.at[ks[i]], load_sem.at[i])
        for xx in (2, 1, 3, 0):
            for j in range(2):
                col = pl.multiple_of((2 * j + 1 - core) * HD, HD)
                start(
                    fv.at[ks[i], xs[xx], :, pl.ds(col, HD)],
                    fr.at[ks[i], xs[xx], :, pl.ds(j * HD, HD)],
                    f_send.at[0],
                    f_recv.at[i],
                    device(x, y, 1 - core, par),
                )

    await_bytes(kv.at[pl.ds(1, 3)], key_sem.at[1])
    for r in range(2):
        for f in range(2):
            lhs[r * HD : (r + 1) * HD, f * HD : (f + 1) * HD] = kv[2 * r + f].T

    lane = lax.broadcasted_iota(jnp.int32, (HD, HD), 1)
    kept = jnp.logical_and(lane >= HALF * par, lane < HALF * par + HALF)

    def tiles(k, dest, j):
        own_lanes = pl.ds(pl.multiple_of((2 * j + core) * HD, HD), HD)
        other_lanes = pl.ds(pl.multiple_of(j * HD, HD), HD)
        return jnp.concatenate([fv[k, dest, :, own_lanes], fr[k, dest, :, other_lanes]], axis=0)

    def partial_pair(k, dest_low, j_low, dest_high, j_high):
        rhs = jnp.concatenate([tiles(k, dest_low, j_low), tiles(k, dest_high, j_high)], axis=1)
        both = jnp.dot(lhs[...], rhs, preferred_element_type=jnp.float32)
        both = both[:HD] + both[HD:]
        low, high = both[:, :HD], both[:, HD:]
        still = jnp.where(par == 0, low, high)
        moved = jnp.where(par == 0, high, low)
        return jnp.where(kept, still, pltpu.roll(moved, HALF, axis=1))

    def partial_for(k, dest):
        return partial_pair(k, dest, 0, dest, 1)

    near = (x + 1 - 2 * lax.rem(x, 2), 3 - x)
    halves = (pl.ds(0, HALF), pl.ds(HALF, HALF))

    def send_far(i):
        await_bytes(fr.at[ks[i]], f_recv.at[i])
        sf[i] = partial_for(ks[i], xs[2])
        for h in range(2):
            start(
                sf.at[i, halves[h]], rx.at[0, i, h], x_send.at[0], x_recv.at[0, i, h],
                device(near[h], y, core, par),
            )

    def send_near(i):
        for a in range(2):
            pn[i, a] = partial_for(ks[i], near[a])
        for h in range(2):
            start(
                pn.at[i, h, halves[h]], rx.at[1, i, h], x_send.at[0], x_recv.at[1, i, h],
                device(near[h], y, core, par),
            )

    def step_two(i):
        for h in range(2):
            await_bytes(rx.at[0, i, h], x_recv.at[0, i, h])
            fw[i, h] = pn[i, 1 - h, halves[h], :] + rx[0, i, h]
            start(
                fw.at[i, h], rx.at[2, i, h], x_send.at[0], x_recv.at[2, i, h],
                device(near[1 - h], y, core, par),
            )

    def own(i):
        px[i] = partial_for(ks[i], x)

    def finish(i):
        for stage in (1, 2):
            for h in range(2):
                await_bytes(rx.at[stage, i, h], x_recv.at[stage, i, h])
        total = px[i] + (rx[1, i] + rx[2, i]).reshape(HD, HD)
        ys[i] = total.T
        for j in range(2):
            yv = 2 * ks[i] + j
            start(ys.at[i, halves[j]], yr.at[y], y_send.at[0], y_recv.at[y], device(x, yv, core, par))

    mine = lax.rem(y, 2)
    beside = 2 * ky + 1 - mine
    last = chunks - 1

    def send_pair():
        await_bytes(fr.at[ks[last]], f_recv.at[last])
        for m in range(2):
            sy[m] = partial_pair(ks[last], xs[m], 1 - mine, xs[m + 2], 1 - mine)
            start(sy.at[m], ry.at[m], p_send.at[0], p_recv.at[m], device(x, beside, core, par))

    def keep_pair():
        for m in range(2):
            sk[m] = partial_pair(ks[last], xs[m], mine, xs[m + 2], mine)

    def spread_pair():
        for m in (0, 1):
            await_bytes(ry.at[m], p_recv.at[m])
            qs[m] = (sk[m] + ry[m]).T
            for d in ((2,), (1, 3))[m]:
                start(
                    qs.at[m, halves[d // 2]], xd.at[d - 1], d_send.at[0], d_recv.at[d - 1],
                    device(xs[d], y, core, par),
                )

    main = range(last)
    if chunks == 4:
        send_far(0)
        send_far(1)
        send_pair()
        send_near(0)
        send_far(2)
        step_two(0)
        send_near(1)
        step_two(1)
        send_near(2)
        for i in main:
            own(i)
        step_two(2)
        keep_pair()
        finish(0)
        spread_pair()
        finish(1)
        finish(2)
    else:
        send_pair()
        for i in main:
            send_far(i)
            send_near(i)
        for i in main:
            step_two(i)
            own(i)
        keep_pair()
        for i in main:
            finish(i)
        spread_pair()

    mom_load.wait()
    grads = qs[0, halves[0], :]
    for i in main:
        for j in range(2):
            yv = 2 * ks[i] + j
            await_bytes(yr.at[yv], y_recv.at[yv])
            grads = grads + yr[yv]
    for d in (1, 3, 2):
        await_bytes(xd.at[d - 1], d_recv.at[d - 1])
        grads = grads + xd[d - 1]

    grads_out[...] = grads
    blend = grads + retain * (retain * mv[...] + grads)
    contract = (((0,), (0,)), ((), ()))
    gs[...] = lax.dot_general(
        blend, blend, contract, precision=PRECISE, preferred_element_type=jnp.float32
    )

    def piece(b):
        return pl.ds(pl.multiple_of(b * 8, 8), 8)

    for xx, cc, pp in others:
        start(
            gs.at[piece(number(xx, cc, pp))], gr.at[member], g_send.at[0], g_recv.at[0],
            device(xx, y, cc, pp),
        )
    gr[member] = gs[piece(member), :]
    await_bytes(gr.at[pl.ds(0, 15)], g_recv.at[0])
    hr[y] = jnp.sum(gr[...], axis=0)
    for d in far_first:
        start(hr.at[y], hr.at[y], g_send.at[1], g_recv.at[1], device(x, yy[d], core, par))
    await_bytes(hr.at[pl.ds(0, ny - 1)], g_recv.at[1])
    ag[member] = jnp.sum(hr[...], axis=0)
    for xx, cc, pp in others:
        start(
            ag.at[member], ag.at[member], g_send.at[2], g_recv.at[2], device(xx, y, cc, pp)
        )
    await_bytes(ag.at[pl.ds(0, 15)], g_recv.at[2])

    gram = ag[...].reshape(HD, HD)
    row = lax.broadcasted_iota(jnp.int32, (HD, HD), 0)
    identity = jnp.where(row == lane, 1.0, 0.0).astype(jnp.float32)
    total = jnp.sum(gram * identity, axis=(0, 1), keepdims=True)
    inverse = 1.0 / (jnp.sqrt(total) + epsilon)

    def parts(a):
        first_part = a.astype(jnp.bfloat16)
        rest = a - first_part.astype(jnp.float32)
        second_part = rest.astype(jnp.bfloat16)
        third_part = (rest - second_part.astype(jnp.float32)).astype(jnp.bfloat16)
        return first_part, second_part, third_part

    def dot(a, b):
        a1, a2, a3 = a
        b1, b2, b3 = b
        m = a1.shape[0]
        upper = jnp.concatenate([a1, a2], axis=0)
        high = jnp.dot(
            jnp.concatenate([upper, upper], axis=1),
            jnp.concatenate([b1, b2], axis=0),
            preferred_element_type=jnp.float32,
        )
        low = jnp.dot(
            jnp.concatenate([a1, a3], axis=1),
            jnp.concatenate([b3, b1], axis=0),
            preferred_element_type=jnp.float32,
        )
        return high[:m] + (high[m:] + low)

    state = blend * inverse
    gram = gram * (inverse * inverse)
    for step in range(ITERS):
        split = parts(gram)
        square = dot(split, split)
        poly = parts(first_coef * identity + second_coef * gram + third_coef * square)
        if step < ITERS - 1:
            both = [
                jnp.concatenate([g, t], axis=0) for g, t in zip(split, parts(state))
            ]
            both = dot(both, poly)
            state = both[HD:]
            gram = dot(parts(both[:HD]), poly)
        else:
            state = dot(parts(state), poly)
    state_out[...] = state

    await_bytes(kv.at[pl.ds(1, 3)], key_sem.at[0])
    await_bytes(fr, f_send.at[0])
    await_bytes(rx, x_send.at[0])
    await_bytes(yr.at[pl.ds(0, ny - 2)], y_send.at[0])
    await_bytes(ry, p_send.at[0])
    await_bytes(xd, d_send.at[0])
    await_bytes(gr.at[pl.ds(0, 15)], g_send.at[0])
    await_bytes(hr.at[pl.ds(0, ny - 1)], g_send.at[1])
    await_bytes(ag.at[pl.ds(0, 15)], g_send.at[2])


def on_device(features, key_partials, momentum):
    ny = lax.axis_size("fsdp") // (2 * NX)
    chunks = ny // 2
    main = chunks - 1
    f32, bf16 = jnp.float32, jnp.bfloat16
    dma = pltpu.SemaphoreType.DMA
    block = jax.ShapeDtypeStruct((HALF, HD), f32)
    hbm = pl.BlockSpec(memory_space=pltpu.HBM)
    vmem = pl.BlockSpec(memory_space=pltpu.VMEM)
    moment = momentum[:, 0, :]

    def body(*refs):
        step_kernel(ny, *refs)

    state, grads = pl.pallas_call(
        body,
        name="muon_step",
        out_shape=(block, block),
        in_specs=[hbm] * 3,
        out_specs=(vmem, vmem),
        scratch_shapes=[
            pltpu.VMEM((chunks, NX, HD, 4 * HD), bf16),
            pltpu.VMEM((chunks, NX, HD, 2 * HD), bf16),
            pltpu.VMEM((4, HD, HD), bf16),
            pltpu.VMEM((2 * HD, 2 * HD), bf16),
            pltpu.VMEM((HALF, HD), f32),
            pltpu.VMEM((main, HD, HD), f32),
            pltpu.VMEM((main, 2, HD, HD), f32),
            pltpu.VMEM((main, HD, HD), f32),
            pltpu.VMEM((3, main, 2, HALF, HD), f32),
            pltpu.VMEM((main, 2, HALF, HD), f32),
            pltpu.VMEM((main, HD, HD), f32),
            pltpu.VMEM((ny, HALF, HD), f32),
            pltpu.VMEM((2, HD, HD), f32),
            pltpu.VMEM((2, HD, HD), f32),
            pltpu.VMEM((2, HD, HD), f32),
            pltpu.VMEM((2, HD, HD), f32),
            pltpu.VMEM((NX - 1, HALF, HD), f32),
            pltpu.VMEM((HD, HD), f32),
            pltpu.VMEM((16, 8, HD), f32),
            pltpu.VMEM((ny, 8, HD), f32),
            pltpu.VMEM((16, 8, HD), f32),
            dma((chunks + 2,)),
            dma((2,)),
            dma((1,)), dma((chunks,)),
            dma((1,)), dma((3, main, 2)),
            dma((1,)), dma((ny,)),
            dma((1,)), dma((2,)),
            dma((1,)), dma((NX - 1,)),
            dma((3,)), dma((3,)),
        ],
        compiler_params=pltpu.CompilerParams(
            collective_id=0, has_side_effects=True, vmem_limit_bytes=16 * 1024 * 1024
        ),
    )(*(pltpu.with_memory_space_constraint(v, pltpu.HBM) for v in (features, key_partials[:, 0, :], moment)))
    update = shrink * math.sqrt(D_W) * state
    return (update[:, None, :], (retain * moment + grads)[:, None, :])


def solution(mesh):
    placed = (P("fsdp", None), P("fsdp", "tp", None), P("fsdp", "tp", None))
    return jax.shard_map(
        on_device,
        mesh=mesh,
        in_specs=placed,
        out_specs=(P("fsdp", "tp", None), P("fsdp", "tp", None)),
        check_vma=False,
    )
```

```python
import math

import jax
import jax.numpy as jnp
from jax import lax
from jax.experimental import pallas as pl
from jax.experimental.pallas import tpu as pltpu
from jax.sharding import PartitionSpec as P

D_W = 8192
ITERS = 5
NX = 4
HD = 128
HALF = 64

retain = 0.95
first_coef = 3.4445
second_coef = -4.775
third_coef = 2.0315
epsilon = 1e-07
shrink = 0.2

MESH = pl.DeviceIdType.MESH
PRECISE = lax.Precision.HIGHEST


def chunk_order(chunks):
    return {1: (0,), 2: (1, 0), 4: (2, 1, 3, 0)}[chunks]


def step_kernel(
    ny, feat, keys, mom, state_out, grads_out,
    fv, fr, kv, lhs, mv, sf, pn, px, rx, fw, ys, yr, sy, ry, sk, qs, xd, gs, gr, hr, ag,
    load_sem, key_sem, f_send, f_recv, x_send, x_recv, y_send, y_recv, p_send, p_recv, d_send, d_recv,
    g_send, g_recv,
):
    chunks = ny // 2
    order = chunk_order(chunks)
    me = lax.axis_index("fsdp")
    z = lax.axis_index("tp")
    core = lax.rem(me, 2)
    chip = lax.div(me, 2)
    y = lax.rem(chip, ny)
    x = lax.div(chip, ny)
    par = lax.rem(z, 2)
    ky = lax.div(y, 2)
    zpair = z - par

    xs = [x] + [lax.rem(x + d, NX) for d in range(1, NX)]
    yy = [y] + [lax.rem(y + d, ny) for d in range(1, ny)]
    cs = (core, 1 - core)
    ps = (par, 1 - par)

    def device(xx, yv, cc, pp):
        return ((xx * ny + yv) * 2 + cc, zpair + pp)

    def number(xx, cc, pp):
        return (xx * 2 + cc) * 2 + pp

    member = number(x, core, par)
    others = [
        (xs[dx], cs[dc], ps[dp])
        for dx in (2, 1, 3, 0)
        for dp in (1, 0)
        for dc in (1, 0)
        if (dx, dp, dc) != (0, 0, 0)
    ]
    far_first = sorted(range(1, ny), key=lambda d: -min(d, ny - d))

    def start(src, dst, send_sem, recv_sem, target):
        pltpu.make_async_remote_copy(
            src_ref=src,
            dst_ref=dst,
            send_sem=send_sem,
            recv_sem=recv_sem,
            device_id=target,
            device_id_type=MESH,
        ).start()

    def await_bytes(ref, sem):
        pltpu.make_async_copy(ref, ref, sem).wait()

    key_load = pltpu.make_async_copy(keys, kv.at[0], load_sem.at[chunks])
    key_load.start()
    barrier = pltpu.get_barrier_semaphore()
    for d in far_first:
        pl.semaphore_signal(
            barrier, inc=1, device_id=device(x, yy[d], core, par), device_id_type=MESH
        )
    for xx, cc, pp in others:
        pl.semaphore_signal(barrier, inc=1, device_id=device(xx, y, cc, pp), device_id_type=MESH)

    def chunk(i):
        return lax.rem(ky + order[i], chunks)

    ks = [chunk(i) for i in range(chunks)]

    wide = 4 * HD
    for i in range(chunks):
        for xx in range(NX):
            col = pl.multiple_of((xx * ny + 2 * ks[i]) * 2 * HD, wide)
            pltpu.make_async_copy(
                feat.at[:, pl.ds(col, wide)], fv.at[ks[i], xx], load_sem.at[i]
            ).start()
    mom_load = pltpu.make_async_copy(mom, mv, load_sem.at[chunks + 1])
    mom_load.start()

    key_load.wait()
    pl.semaphore_wait(barrier, 15 + ny - 1)

    for cc in range(2):
        apart = (core + cc) - 2 * core * cc
        start(kv.at[0], kv.at[2 + apart], key_sem.at[0], key_sem.at[1], device(x, y, cc, ps[1]))
    start(kv.at[0], kv.at[1], key_sem.at[0], key_sem.at[1], device(x, y, cs[1], par))
    for i in range(chunks):
        await_bytes(fv.at[ks[i]], load_sem.at[i])
        for xx in (2, 1, 3, 0):
            for j in range(2):
                col = pl.multiple_of((2 * j + 1 - core) * HD, HD)
                start(
                    fv.at[ks[i], xs[xx], :, pl.ds(col, HD)],
                    fr.at[ks[i], xs[xx], :, pl.ds(j * HD, HD)],
                    f_send.at[0],
                    f_recv.at[i],
                    device(x, y, 1 - core, par),
                )

    await_bytes(kv.at[pl.ds(1, 3)], key_sem.at[1])
    for r in range(2):
        for f in range(2):
            lhs[r * HD : (r + 1) * HD, f * HD : (f + 1) * HD] = kv[2 * r + f].T

    lane = lax.broadcasted_iota(jnp.int32, (HD, HD), 1)
    kept = jnp.logical_and(lane >= HALF * par, lane < HALF * par + HALF)

    def tiles(k, dest, j):
        own_lanes = pl.ds(pl.multiple_of((2 * j + core) * HD, HD), HD)
        other_lanes = pl.ds(pl.multiple_of(j * HD, HD), HD)
        return jnp.concatenate([fv[k, dest, :, own_lanes], fr[k, dest, :, other_lanes]], axis=0)

    def partial_pair(k, dest_low, j_low, dest_high, j_high):
        rhs = jnp.concatenate([tiles(k, dest_low, j_low), tiles(k, dest_high, j_high)], axis=1)
        both = jnp.dot(lhs[...], rhs, preferred_element_type=jnp.float32)
        both = both[:HD] + both[HD:]
        low, high = both[:, :HD], both[:, HD:]
        still = jnp.where(par == 0, low, high)
        moved = jnp.where(par == 0, high, low)
        return jnp.where(kept, still, pltpu.roll(moved, HALF, axis=1))

    def partial_for(k, dest):
        return partial_pair(k, dest, 0, dest, 1)

    near = (x + 1 - 2 * lax.rem(x, 2), 3 - x)
    halves = (pl.ds(0, HALF), pl.ds(HALF, HALF))

    def compute_far(i):
        await_bytes(fr.at[ks[i]], f_recv.at[i])
        sf[i] = partial_for(ks[i], xs[2])

    def send_far(i):
        for h in range(2):
            start(
                sf.at[i, halves[h]], rx.at[0, i, h], x_send.at[0], x_recv.at[0, i, h],
                device(near[h], y, core, par),
            )

    def compute_near(i):
        for a in range(2):
            pn[i, a] = partial_for(ks[i], near[a])

    def send_near(i):
        for h in range(2):
            start(
                pn.at[i, h, halves[h]], rx.at[1, i, h], x_send.at[0], x_recv.at[1, i, h],
                device(near[h], y, core, par),
            )

    def step_two(i):
        for h in range(2):
            await_bytes(rx.at[0, i, h], x_recv.at[0, i, h])
            fw[i, h] = pn[i, 1 - h, halves[h], :] + rx[0, i, h]
            start(
                fw.at[i, h], rx.at[2, i, h], x_send.at[0], x_recv.at[2, i, h],
                device(near[1 - h], y, core, par),
            )

    def own(i):
        px[i] = partial_for(ks[i], x)

    def finish(i):
        for stage in (1, 2):
            for h in range(2):
                await_bytes(rx.at[stage, i, h], x_recv.at[stage, i, h])
        total = px[i] + (rx[1, i] + rx[2, i]).reshape(HD, HD)
        ys[i] = total.T
        for j in range(2):
            yv = 2 * ks[i] + j
            start(ys.at[i, halves[j]], yr.at[y], y_send.at[0], y_recv.at[y], device(x, yv, core, par))

    mine = lax.rem(y, 2)
    beside = 2 * ky + 1 - mine
    last = chunks - 1

    def compute_pair():
        await_bytes(fr.at[ks[last]], f_recv.at[last])
        for m in range(2):
            sy[m] = partial_pair(ks[last], xs[m], 1 - mine, xs[m + 2], 1 - mine)

    def send_pair():
        for m in range(2):
            start(sy.at[m], ry.at[m], p_send.at[0], p_recv.at[m], device(x, beside, core, par))

    def keep_pair():
        for m in range(2):
            sk[m] = partial_pair(ks[last], xs[m], mine, xs[m + 2], mine)

    def spread_pair():
        for m in (0, 1):
            await_bytes(ry.at[m], p_recv.at[m])
            qs[m] = (sk[m] + ry[m]).T
            for d in ((2,), (1, 3))[m]:
                start(
                    qs.at[m, halves[d // 2]], xd.at[d - 1], d_send.at[0], d_recv.at[d - 1],
                    device(xs[d], y, core, par),
                )

    main = range(last)
    compute_far(0)
    send_far(0)
    compute_near(0)
    send_near(0)
    for i in main[1:]:
        compute_far(i)
    for i in main[1:]:
        send_far(i)
    compute_pair()
    send_pair()
    step_two(0)
    for i in main[1:]:
        compute_near(i)
        send_near(i)
    for i in main[1:]:
        step_two(i)
    own(0)
    keep_pair()
    finish(0)
    spread_pair()
    for i in main[1:]:
        own(i)
    for i in main[1:]:
        finish(i)

    mom_load.wait()
    grads = qs[0, halves[0], :]
    for i in main:
        for j in range(2):
            yv = 2 * ks[i] + j
            await_bytes(yr.at[yv], y_recv.at[yv])
            grads = grads + yr[yv]
    for d in (1, 3, 2):
        await_bytes(xd.at[d - 1], d_recv.at[d - 1])
        grads = grads + xd[d - 1]

    grads_out[...] = grads
    blend = grads + retain * (retain * mv[...] + grads)
    contract = (((0,), (0,)), ((), ()))
    gs[...] = lax.dot_general(
        blend, blend, contract, precision=PRECISE, preferred_element_type=jnp.float32
    ).reshape(8, 16, HD)

    owner = x * 2 + par
    owners = [(xs[dx], ps[dp]) for dx in (2, 1, 3, 0) for dp in (1, 0)]
    for xx, pp in owners[:-1]:
        start(
            gs.at[xx * 2 + pp], gr.at[member], g_send.at[0], g_recv.at[0], device(xx, y, 1, pp)
        )

    @pl.when(core == 0)
    def _():
        start(gs.at[owner], gr.at[member], g_send.at[0], g_recv.at[0], device(x, y, 1, par))
        await_bytes(ag, g_recv.at[2])

    @pl.when(core == 1)
    def _():
        gr[member] = gs[owner]
        await_bytes(gr.at[pl.ds(0, 15)], g_recv.at[0])
        hr[y] = jnp.sum(gr[...], axis=0)
        for d in far_first:
            start(hr.at[y], hr.at[y], g_send.at[1], g_recv.at[1], device(x, yy[d], 1, par))
        await_bytes(hr.at[pl.ds(0, ny - 1)], g_recv.at[1])
        ag[owner] = jnp.sum(hr[...], axis=0)
        for xx, cc, pp in others:
            start(ag.at[owner], ag.at[owner], g_send.at[2], g_recv.at[2], device(xx, y, cc, pp))
        await_bytes(ag.at[pl.ds(0, 7)], g_recv.at[2])

    gram = ag[...].reshape(HD, HD)
    row = lax.broadcasted_iota(jnp.int32, (HD, HD), 0)
    identity = jnp.where(row == lane, 1.0, 0.0).astype(jnp.float32)
    total = jnp.sum(gram * identity, axis=(0, 1), keepdims=True)
    inverse = 1.0 / (jnp.sqrt(total) + epsilon)

    def parts(a):
        first_part = a.astype(jnp.bfloat16)
        rest = a - first_part.astype(jnp.float32)
        second_part = rest.astype(jnp.bfloat16)
        third_part = (rest - second_part.astype(jnp.float32)).astype(jnp.bfloat16)
        return first_part, second_part, third_part

    def dot(a, b):
        a1, a2, a3 = a
        b1, b2, b3 = b
        m = a1.shape[0]
        upper = jnp.concatenate([a1, a2], axis=0)
        high = jnp.dot(
            jnp.concatenate([upper, upper], axis=1),
            jnp.concatenate([b1, b2], axis=0),
            preferred_element_type=jnp.float32,
        )
        low = jnp.dot(
            jnp.concatenate([a1, a3], axis=1),
            jnp.concatenate([b3, b1], axis=0),
            preferred_element_type=jnp.float32,
        )
        return high[:m] + (high[m:] + low)

    state = blend * inverse
    gram = gram * (inverse * inverse)
    for step in range(ITERS):
        split = parts(gram)
        square = dot(split, split)
        poly = parts(first_coef * identity + second_coef * gram + third_coef * square)
        if step < ITERS - 1:
            both = [
                jnp.concatenate([g, t], axis=0) for g, t in zip(split, parts(state))
            ]
            both = dot(both, poly)
            state = both[HD:]
            gram = dot(parts(both[:HD]), poly)
        else:
            state = dot(parts(state), poly)
    state_out[...] = state

    await_bytes(kv.at[pl.ds(1, 3)], key_sem.at[0])
    await_bytes(fr, f_send.at[0])
    await_bytes(rx, x_send.at[0])
    await_bytes(yr.at[pl.ds(0, ny - 2)], y_send.at[0])
    await_bytes(ry, p_send.at[0])
    await_bytes(xd, d_send.at[0])
    await_bytes(gs.at[pl.ds(0, 7)], g_send.at[0])

    @pl.when(core == 0)
    def _():
        await_bytes(gs.at[0], g_send.at[0])

    @pl.when(core == 1)
    def _():
        await_bytes(hr.at[pl.ds(0, ny - 1)], g_send.at[1])
        await_bytes(gr.at[pl.ds(0, 15)], g_send.at[2])


def on_device(features, key_partials, momentum):
    ny = lax.axis_size("fsdp") // (2 * NX)
    chunks = ny // 2
    main = chunks - 1
    f32, bf16 = jnp.float32, jnp.bfloat16
    dma = pltpu.SemaphoreType.DMA
    block = jax.ShapeDtypeStruct((HALF, HD), f32)
    hbm = pl.BlockSpec(memory_space=pltpu.HBM)
    vmem = pl.BlockSpec(memory_space=pltpu.VMEM)
    moment = momentum[:, 0, :]

    def body(*refs):
        step_kernel(ny, *refs)

    state, grads = pl.pallas_call(
        body,
        name="muon_step",
        out_shape=(block, block),
        in_specs=[hbm] * 3,
        out_specs=(vmem, vmem),
        scratch_shapes=[
            pltpu.VMEM((chunks, NX, HD, 4 * HD), bf16),
            pltpu.VMEM((chunks, NX, HD, 2 * HD), bf16),
            pltpu.VMEM((4, HD, HD), bf16),
            pltpu.VMEM((2 * HD, 2 * HD), bf16),
            pltpu.VMEM((HALF, HD), f32),
            pltpu.VMEM((main, HD, HD), f32),
            pltpu.VMEM((main, 2, HD, HD), f32),
            pltpu.VMEM((main, HD, HD), f32),
            pltpu.VMEM((3, main, 2, HALF, HD), f32),
            pltpu.VMEM((main, 2, HALF, HD), f32),
            pltpu.VMEM((main, HD, HD), f32),
            pltpu.VMEM((ny, HALF, HD), f32),
            pltpu.VMEM((2, HD, HD), f32),
            pltpu.VMEM((2, HD, HD), f32),
            pltpu.VMEM((2, HD, HD), f32),
            pltpu.VMEM((2, HD, HD), f32),
            pltpu.VMEM((NX - 1, HALF, HD), f32),
            pltpu.VMEM((8, 16, HD), f32),
            pltpu.VMEM((16, 16, HD), f32),
            pltpu.VMEM((ny, 16, HD), f32),
            pltpu.VMEM((8, 16, HD), f32),
            dma((chunks + 2,)),
            dma((2,)),
            dma((1,)), dma((chunks,)),
            dma((1,)), dma((3, main, 2)),
            dma((1,)), dma((ny,)),
            dma((1,)), dma((2,)),
            dma((1,)), dma((NX - 1,)),
            dma((3,)), dma((3,)),
        ],
        compiler_params=pltpu.CompilerParams(
            collective_id=0, has_side_effects=True, vmem_limit_bytes=16 * 1024 * 1024
        ),
    )(*(pltpu.with_memory_space_constraint(v, pltpu.HBM) for v in (features, key_partials[:, 0, :], moment)))
    update = shrink * math.sqrt(D_W) * state
    return (update[:, None, :], (retain * moment + grads)[:, None, :])


def solution(mesh):
    placed = (P("fsdp", None), P("fsdp", "tp", None), P("fsdp", "tp", None))
    return jax.shard_map(
        on_device,
        mesh=mesh,
        in_specs=placed,
        out_specs=(P("fsdp", "tp", None), P("fsdp", "tp", None)),
        check_vma=False,
    )
```

```python
import math

import jax
import jax.numpy as jnp
from jax import lax
from jax.experimental import pallas as pl
from jax.experimental.pallas import tpu as pltpu
from jax.sharding import PartitionSpec as P

D_W = 8192
ITERS = 5
NX = 4
HD = 128
HALF = 64

retain = 0.95
first_coef = 3.4445
second_coef = -4.775
third_coef = 2.0315
epsilon = 1e-07
shrink = 0.2

MESH = pl.DeviceIdType.MESH
PRECISE = lax.Precision.HIGHEST


def chunk_order(chunks):
    return {1: (0,), 2: (1, 0), 4: (2, 1, 3, 0)}[chunks]


def step_kernel(
    ny, feat, keys, mom, state_out, grads_out,
    fv, fr, kv, lhs, mv, sf, pn, px, rx, fw, ys, yr, sy, ry, sk, qs, xd, gs, gr, hr, ag,
    load_sem, key_sem, f_send, f_recv, x_send, x_recv, far_recv, y_send, y_recv, p_send, p_recv, d_send, d_recv,
    g_send, g_recv,
):
    chunks = ny // 2
    order = chunk_order(chunks)
    me = lax.axis_index("fsdp")
    z = lax.axis_index("tp")
    core = lax.rem(me, 2)
    chip = lax.div(me, 2)
    y = lax.rem(chip, ny)
    x = lax.div(chip, ny)
    par = lax.rem(z, 2)
    ky = lax.div(y, 2)
    mine = lax.rem(y, 2)
    zpair = z - par

    xs = [x] + [lax.rem(x + d, NX) for d in range(1, NX)]
    yy = [y] + [lax.rem(y + d, ny) for d in range(1, ny)]
    cs = (core, 1 - core)
    ps = (par, 1 - par)

    def device(xx, yv, cc, pp):
        return ((xx * ny + yv) * 2 + cc, zpair + pp)

    def number(xx, cc, pp):
        return (xx * 2 + cc) * 2 + pp

    member = number(x, core, par)
    others = [
        (xs[dx], cs[dc], ps[dp])
        for dx in (2, 1, 3, 0)
        for dp in (1, 0)
        for dc in (1, 0)
        if (dx, dp, dc) != (0, 0, 0)
    ]
    far_first = sorted(range(1, ny), key=lambda d: -min(d, ny - d))

    def start(src, dst, send_sem, recv_sem, target):
        pltpu.make_async_remote_copy(
            src_ref=src,
            dst_ref=dst,
            send_sem=send_sem,
            recv_sem=recv_sem,
            device_id=target,
            device_id_type=MESH,
        ).start()

    def await_bytes(ref, sem):
        pltpu.make_async_copy(ref, ref, sem).wait()

    key_load = pltpu.make_async_copy(keys, kv.at[0], load_sem.at[chunks])
    key_load.start()
    barrier = pltpu.get_barrier_semaphore()
    for d in far_first:
        pl.semaphore_signal(
            barrier, inc=1, device_id=device(x, yy[d], core, par), device_id_type=MESH
        )
    for xx, cc, pp in others:
        pl.semaphore_signal(barrier, inc=1, device_id=device(xx, y, cc, pp), device_id_type=MESH)

    def chunk(i):
        return lax.rem(ky + order[i], chunks)

    ks = [chunk(i) for i in range(chunks)]

    wide = 4 * HD
    for i in range(chunks):
        for xx in range(NX):
            col = pl.multiple_of((xx * ny + 2 * ks[i]) * 2 * HD, wide)
            pltpu.make_async_copy(
                feat.at[:, pl.ds(col, wide)], fv.at[ks[i], xx], load_sem.at[i]
            ).start()
    mom_load = pltpu.make_async_copy(mom, mv, load_sem.at[chunks + 1])
    mom_load.start()

    key_load.wait()
    pl.semaphore_wait(barrier, 15 + ny - 1)

    for cc in range(2):
        apart = (core + cc) - 2 * core * cc
        start(kv.at[0], kv.at[2 + apart], key_sem.at[0], key_sem.at[1], device(x, y, cc, ps[1]))
    start(kv.at[0], kv.at[1], key_sem.at[0], key_sem.at[1], device(x, y, cs[1], par))
    for i in range(chunks):
        await_bytes(fv.at[ks[i]], load_sem.at[i])
        for xx in (2, 1, 3, 0):
            for j in range(2):
                col = pl.multiple_of((2 * j + 1 - core) * HD, HD)
                start(
                    fv.at[ks[i], xs[xx], :, pl.ds(col, HD)],
                    fr.at[ks[i], xs[xx], :, pl.ds(j * HD, HD)],
                    f_send.at[0],
                    f_recv.at[i],
                    device(x, y, 1 - core, par),
                )

    await_bytes(kv.at[pl.ds(1, 3)], key_sem.at[1])
    for r in range(2):
        for f in range(2):
            lhs[r * HD : (r + 1) * HD, f * HD : (f + 1) * HD] = kv[2 * r + f].T

    lane = lax.broadcasted_iota(jnp.int32, (HD, HD), 1)
    kept = jnp.logical_and(lane >= HALF * par, lane < HALF * par + HALF)

    def tiles(k, dest, j):
        own_lanes = pl.ds(pl.multiple_of((2 * j + core) * HD, HD), HD)
        other_lanes = pl.ds(pl.multiple_of(j * HD, HD), HD)
        return jnp.concatenate([fv[k, dest, :, own_lanes], fr[k, dest, :, other_lanes]], axis=0)

    def partial_pair(k, dest_low, j_low, dest_high, j_high):
        rhs = jnp.concatenate([tiles(k, dest_low, j_low), tiles(k, dest_high, j_high)], axis=1)
        both = jnp.dot(lhs[...], rhs, preferred_element_type=jnp.float32)
        both = both[:HD] + both[HD:]
        low, high = both[:, :HD], both[:, HD:]
        still = jnp.where(par == 0, low, high)
        moved = jnp.where(par == 0, high, low)
        return jnp.where(kept, still, pltpu.roll(moved, HALF, axis=1))

    def partial_for(k, dest):
        return partial_pair(k, dest, 0, dest, 1)

    near = (x + 1 - 2 * lax.rem(x, 2), 3 - x)
    halves = (pl.ds(0, HALF), pl.ds(HALF, HALF))

    def compute_far(i):
        await_bytes(fr.at[ks[i]], f_recv.at[i])
        sf[i] = partial_for(ks[i], xs[2])

    def send_far(i):
        for h in range(2):
            start(
                sf.at[i, halves[h]], rx.at[0, i, h], x_send.at[0], far_recv.at[i, h],
                device(near[h], y, core, par),
            )

    def compute_near(i):
        for a in range(2):
            pn[i, a] = partial_for(ks[i], near[a])

    def send_near(i):
        for h in range(2):
            start(
                pn.at[i, h, halves[h]], rx.at[1, i, h], x_send.at[0], x_recv.at[i],
                device(near[h], y, core, par),
            )

    def step_two(i):
        for h in range(2):
            await_bytes(rx.at[0, i, h], far_recv.at[i, h])
            fw[i, h] = pn[i, 1 - h, halves[h], :] + rx[0, i, h]
            start(
                fw.at[i, h], rx.at[2, i, h], x_send.at[0], x_recv.at[i],
                device(near[1 - h], y, core, par),
            )

    def own(i):
        px[i] = partial_for(ks[i], x)

    def finish(i):
        await_bytes(ry, x_recv.at[i])
        total = px[i] + (rx[1, i] + rx[2, i]).reshape(HD, HD)
        ys[i] = total.T
        farther = {0: 0, 1: 1, 2: mine, 3: 0}[order[i]]
        for j in (farther, 1 - farther):
            rows = pl.ds(pl.multiple_of(j * HALF, HALF), HALF)
            start(
                ys.at[i, rows], yr.at[y], y_send.at[0], y_recv.at[0],
                device(x, 2 * ks[i] + j, core, par),
            )

    beside = 2 * ky + 1 - mine
    last = chunks - 1

    def compute_pair():
        await_bytes(fr.at[ks[last]], f_recv.at[last])
        for m in range(2):
            sy[m] = partial_pair(ks[last], xs[m], 1 - mine, xs[m + 2], 1 - mine)

    def send_pair():
        for m in range(2):
            start(sy.at[m], ry.at[m], p_send.at[0], p_recv.at[m], device(x, beside, core, par))

    def keep_pair():
        for m in range(2):
            sk[m] = partial_pair(ks[last], xs[m], mine, xs[m + 2], mine)

    def spread_pair():
        for m in (0, 1):
            await_bytes(ry.at[m], p_recv.at[m])
            qs[m] = (sk[m] + ry[m]).T
            for d in ((2,), (1, 3))[m]:
                start(
                    qs.at[m, halves[d // 2]], xd.at[d - 1], d_send.at[0], d_recv.at[0],
                    device(xs[d], y, core, par),
                )

    main = range(last)
    compute_far(0)
    send_far(0)
    compute_near(0)
    send_near(0)
    for i in main[1:]:
        compute_far(i)
    for i in main[1:]:
        send_far(i)
    compute_pair()
    send_pair()
    step_two(0)
    for i in main[1:]:
        compute_near(i)
        send_near(i)
    for i in main[1:]:
        step_two(i)
    keep_pair()
    own(0)
    finish(0)
    spread_pair()
    for i in main[1:]:
        own(i)
    for i in main[1:]:
        finish(i)

    mom_load.wait()
    grads = qs[0, halves[0], :]
    await_bytes(xd, d_recv.at[0])
    for d in (1, 2, 3):
        grads = grads + xd[d - 1]
    await_bytes(yr.at[pl.ds(0, ny - 2)], y_recv.at[0])
    for i in main:
        for j in range(2):
            grads = grads + yr[2 * ks[i] + j]

    grads_out[...] = grads
    blend = grads + retain * (retain * mv[...] + grads)
    contract = (((0,), (0,)), ((), ()))
    gs[...] = lax.dot_general(
        blend, blend, contract, precision=PRECISE, preferred_element_type=jnp.float32
    ).reshape(8, 16, HD)

    owner = x * 2 + par
    owners = [(xs[dx], ps[dp]) for dx in (2, 1, 3, 0) for dp in (1, 0)]
    for xx, pp in owners[:-1]:
        start(
            gs.at[xx * 2 + pp], gr.at[member], g_send.at[0], g_recv.at[0], device(xx, y, 1, pp)
        )

    @pl.when(core == 0)
    def _():
        start(gs.at[owner], gr.at[member], g_send.at[0], g_recv.at[0], device(x, y, 1, par))
        await_bytes(ag, g_recv.at[2])

    @pl.when(core == 1)
    def _():
        gr[member] = gs[owner]
        await_bytes(gr.at[pl.ds(0, 15)], g_recv.at[0])
        hr[y] = jnp.sum(gr[...], axis=0)
        for d in far_first:
            start(hr.at[y], hr.at[y], g_send.at[1], g_recv.at[1], device(x, yy[d], 1, par))
        await_bytes(hr.at[pl.ds(0, ny - 1)], g_recv.at[1])
        ag[owner] = jnp.sum(hr[...], axis=0)
        for xx, cc, pp in others:
            start(ag.at[owner], ag.at[owner], g_send.at[2], g_recv.at[2], device(xx, y, cc, pp))
        await_bytes(ag.at[pl.ds(0, 7)], g_recv.at[2])

    gram = ag[...].reshape(HD, HD)
    row = lax.broadcasted_iota(jnp.int32, (HD, HD), 0)
    identity = jnp.where(row == lane, 1.0, 0.0).astype(jnp.float32)
    total = jnp.sum(gram * identity, axis=(0, 1), keepdims=True)
    inverse = 1.0 / (jnp.sqrt(total) + epsilon)

    def parts(a):
        first_part = a.astype(jnp.bfloat16)
        rest = a - first_part.astype(jnp.float32)
        second_part = rest.astype(jnp.bfloat16)
        third_part = (rest - second_part.astype(jnp.float32)).astype(jnp.bfloat16)
        return first_part, second_part, third_part

    def dot(a, b):
        a1, a2, a3 = a
        b1, b2, b3 = b
        m = a1.shape[0]
        upper = jnp.concatenate([a1, a2], axis=0)
        high = jnp.dot(
            jnp.concatenate([upper, upper], axis=1),
            jnp.concatenate([b1, b2], axis=0),
            preferred_element_type=jnp.float32,
        )
        low = jnp.dot(
            jnp.concatenate([a1, a3], axis=1),
            jnp.concatenate([b3, b1], axis=0),
            preferred_element_type=jnp.float32,
        )
        return high[:m] + (high[m:] + low)

    state = blend * inverse
    gram = gram * (inverse * inverse)
    for step in range(ITERS):
        split = parts(gram)
        square = dot(split, split)
        poly = parts(first_coef * identity + second_coef * gram + third_coef * square)
        if step < ITERS - 1:
            both = [
                jnp.concatenate([g, t], axis=0) for g, t in zip(split, parts(state))
            ]
            both = dot(both, poly)
            state = both[HD:]
            gram = dot(parts(both[:HD]), poly)
        else:
            state = dot(parts(state), poly)
    state_out[...] = state

    await_bytes(kv.at[pl.ds(1, 3)], key_sem.at[0])
    await_bytes(fr, f_send.at[0])
    await_bytes(rx, x_send.at[0])
    await_bytes(yr.at[pl.ds(0, ny - 2)], y_send.at[0])
    await_bytes(ry, p_send.at[0])
    await_bytes(xd, d_send.at[0])
    await_bytes(gs.at[pl.ds(0, 7)], g_send.at[0])

    @pl.when(core == 0)
    def _():
        await_bytes(gs.at[0], g_send.at[0])

    @pl.when(core == 1)
    def _():
        await_bytes(hr.at[pl.ds(0, ny - 1)], g_send.at[1])
        await_bytes(gr.at[pl.ds(0, 15)], g_send.at[2])


def on_device(features, key_partials, momentum):
    ny = lax.axis_size("fsdp") // (2 * NX)
    chunks = ny // 2
    main = chunks - 1
    f32, bf16 = jnp.float32, jnp.bfloat16
    dma = pltpu.SemaphoreType.DMA
    block = jax.ShapeDtypeStruct((HALF, HD), f32)
    hbm = pl.BlockSpec(memory_space=pltpu.HBM)
    vmem = pl.BlockSpec(memory_space=pltpu.VMEM)
    moment = momentum[:, 0, :]

    def body(*refs):
        step_kernel(ny, *refs)

    state, grads = pl.pallas_call(
        body,
        name="muon_step",
        out_shape=(block, block),
        in_specs=[hbm] * 3,
        out_specs=(vmem, vmem),
        scratch_shapes=[
            pltpu.VMEM((chunks, NX, HD, 4 * HD), bf16),
            pltpu.VMEM((chunks, NX, HD, 2 * HD), bf16),
            pltpu.VMEM((4, HD, HD), bf16),
            pltpu.VMEM((2 * HD, 2 * HD), bf16),
            pltpu.VMEM((HALF, HD), f32),
            pltpu.VMEM((main, HD, HD), f32),
            pltpu.VMEM((main, 2, HD, HD), f32),
            pltpu.VMEM((main, HD, HD), f32),
            pltpu.VMEM((3, main, 2, HALF, HD), f32),
            pltpu.VMEM((main, 2, HALF, HD), f32),
            pltpu.VMEM((main, HD, HD), f32),
            pltpu.VMEM((ny, HALF, HD), f32),
            pltpu.VMEM((2, HD, HD), f32),
            pltpu.VMEM((2, HD, HD), f32),
            pltpu.VMEM((2, HD, HD), f32),
            pltpu.VMEM((2, HD, HD), f32),
            pltpu.VMEM((NX - 1, HALF, HD), f32),
            pltpu.VMEM((8, 16, HD), f32),
            pltpu.VMEM((16, 16, HD), f32),
            pltpu.VMEM((ny, 16, HD), f32),
            pltpu.VMEM((8, 16, HD), f32),
            dma((chunks + 2,)),
            dma((2,)),
            dma((1,)), dma((chunks,)),
            dma((1,)), dma((main,)), dma((main, 2)),
            dma((1,)), dma((1,)),
            dma((1,)), dma((2,)),
            dma((1,)), dma((1,)),
            dma((3,)), dma((3,)),
        ],
        compiler_params=pltpu.CompilerParams(
            collective_id=0, has_side_effects=True, vmem_limit_bytes=16 * 1024 * 1024
        ),
    )(*(pltpu.with_memory_space_constraint(v, pltpu.HBM) for v in (features, key_partials[:, 0, :], moment)))
    update = shrink * math.sqrt(D_W) * state
    return (update[:, None, :], (retain * moment + grads)[:, None, :])


def solution(mesh):
    placed = (P("fsdp", None), P("fsdp", "tp", None), P("fsdp", "tp", None))
    return jax.shard_map(
        on_device,
        mesh=mesh,
        in_specs=placed,
        out_specs=(P("fsdp", "tp", None), P("fsdp", "tp", None)),
        check_vma=False,
    )
```

```python
import math

import jax
import jax.numpy as jnp
from jax import lax
from jax.experimental import pallas as pl
from jax.experimental.pallas import tpu as pltpu
from jax.sharding import PartitionSpec as P

D_W = 8192
ITERS = 5
NX = 4
HD = 128
HALF = 64

retain = 0.95
first_coef = 3.4445
second_coef = -4.775
third_coef = 2.0315
epsilon = 1e-07
shrink = 0.2

MESH = pl.DeviceIdType.MESH
PRECISE = lax.Precision.HIGHEST


def chunk_order(chunks):
    return {1: (0,), 2: (1, 0), 4: (2, 1, 3, 0)}[chunks]


def step_kernel(
    ny, feat, keys, mom, state_out, grads_out,
    fv, fr, kv, lhs, mv, sf, pn, px, rx, fw, ys, yr, sy, ry, sk, qs, xd, gs, gr, hr, ag,
    load_sem, key_sem, f_send, f_recv, x_send, x_recv, far_recv, y_send, y_recv, p_send, p_recv, d_send, d_recv,
    g_send, g_recv,
):
    chunks = ny // 2
    order = chunk_order(chunks)
    me = lax.axis_index("fsdp")
    z = lax.axis_index("tp")
    core = lax.rem(me, 2)
    chip = lax.div(me, 2)
    y = lax.rem(chip, ny)
    x = lax.div(chip, ny)
    par = lax.rem(z, 2)
    ky = lax.div(y, 2)
    mine = lax.rem(y, 2)
    zpair = z - par

    xs = [x] + [lax.rem(x + d, NX) for d in range(1, NX)]
    yy = [y] + [lax.rem(y + d, ny) for d in range(1, ny)]
    cs = (core, 1 - core)
    ps = (par, 1 - par)

    def device(xx, yv, cc, pp):
        return ((xx * ny + yv) * 2 + cc, zpair + pp)

    def number(xx, cc, pp):
        return (xx * 2 + cc) * 2 + pp

    member = number(x, core, par)
    others = [
        (xs[dx], cs[dc], ps[dp])
        for dx in (2, 1, 3, 0)
        for dp in (1, 0)
        for dc in (1, 0)
        if (dx, dp, dc) != (0, 0, 0)
    ]
    far_first = sorted(range(1, ny), key=lambda d: -min(d, ny - d))

    def start(src, dst, send_sem, recv_sem, target):
        pltpu.make_async_remote_copy(
            src_ref=src,
            dst_ref=dst,
            send_sem=send_sem,
            recv_sem=recv_sem,
            device_id=target,
            device_id_type=MESH,
        ).start()

    def await_bytes(ref, sem):
        pltpu.make_async_copy(ref, ref, sem).wait()

    key_load = pltpu.make_async_copy(keys, kv.at[0], load_sem.at[chunks])
    key_load.start()
    barrier = pltpu.get_barrier_semaphore()
    for d in far_first:
        pl.semaphore_signal(
            barrier, inc=1, device_id=device(x, yy[d], core, par), device_id_type=MESH
        )
    for xx, cc, pp in others:
        pl.semaphore_signal(barrier, inc=1, device_id=device(xx, y, cc, pp), device_id_type=MESH)

    def chunk(i):
        return lax.rem(ky + order[i], chunks)

    ks = [chunk(i) for i in range(chunks)]

    wide = 4 * HD
    for i in range(chunks):
        for xx in range(NX):
            col = pl.multiple_of((xx * ny + 2 * ks[i]) * 2 * HD, wide)
            pltpu.make_async_copy(
                feat.at[:, pl.ds(col, wide)], fv.at[ks[i], xx], load_sem.at[i]
            ).start()
    mom_load = pltpu.make_async_copy(mom, mv, load_sem.at[chunks + 1])
    mom_load.start()

    key_load.wait()
    pl.semaphore_wait(barrier, 15 + ny - 1)

    for cc in range(2):
        apart = (core + cc) - 2 * core * cc
        start(kv.at[0], kv.at[2 + apart], key_sem.at[0], key_sem.at[1], device(x, y, cc, ps[1]))
    start(kv.at[0], kv.at[1], key_sem.at[0], key_sem.at[2], device(x, y, cs[1], par))
    for i in range(chunks):
        await_bytes(fv.at[ks[i]], load_sem.at[i])
        for xx in (2, 1, 3, 0):
            for j in range(2):
                col = pl.multiple_of((2 * j + 1 - core) * HD, HD)
                start(
                    fv.at[ks[i], xs[xx], :, pl.ds(col, HD)],
                    fr.at[ks[i], xs[xx], :, pl.ds(j * HD, HD)],
                    f_send.at[0],
                    f_recv.at[i],
                    device(x, y, 1 - core, par),
                )

    await_bytes(kv.at[1], key_sem.at[2])
    for r in range(2):
        if r == 1:
            await_bytes(kv.at[pl.ds(2, 2)], key_sem.at[1])
        for f in range(2):
            lhs[r * HD : (r + 1) * HD, f * HD : (f + 1) * HD] = kv[2 * r + f].T

    lane = lax.broadcasted_iota(jnp.int32, (HD, HD), 1)
    kept = jnp.logical_and(lane >= HALF * par, lane < HALF * par + HALF)

    def tiles(k, dest, j):
        own_lanes = pl.ds(pl.multiple_of((2 * j + core) * HD, HD), HD)
        other_lanes = pl.ds(pl.multiple_of(j * HD, HD), HD)
        return jnp.concatenate([fv[k, dest, :, own_lanes], fr[k, dest, :, other_lanes]], axis=0)

    def partial_pair(k, dest_low, j_low, dest_high, j_high):
        rhs = jnp.concatenate([tiles(k, dest_low, j_low), tiles(k, dest_high, j_high)], axis=1)
        both = jnp.dot(lhs[...], rhs, preferred_element_type=jnp.float32)
        both = both[:HD] + both[HD:]
        low, high = both[:, :HD], both[:, HD:]
        still = jnp.where(par == 0, low, high)
        moved = jnp.where(par == 0, high, low)
        return jnp.where(kept, still, pltpu.roll(moved, HALF, axis=1))

    def partial_for(k, dest):
        return partial_pair(k, dest, 0, dest, 1)

    near = (x + 1 - 2 * lax.rem(x, 2), 3 - x)
    halves = (pl.ds(0, HALF), pl.ds(HALF, HALF))

    def compute_far(i):
        await_bytes(fr.at[ks[i]], f_recv.at[i])
        sf[i] = partial_for(ks[i], xs[2])

    def send_far(i):
        for h in range(2):
            start(
                sf.at[i, halves[h]], rx.at[0, i, h], x_send.at[0], far_recv.at[i, h],
                device(near[h], y, core, par),
            )

    def compute_near(i):
        for a in range(2):
            pn[i, a] = partial_for(ks[i], near[a])

    def send_near(i):
        for h in range(2):
            start(
                pn.at[i, h, halves[h]], rx.at[1, i, h], x_send.at[0], x_recv.at[i],
                device(near[h], y, core, par),
            )

    def step_two(i):
        for h in range(2):
            await_bytes(rx.at[0, i, h], far_recv.at[i, h])
            fw[i, h] = pn[i, 1 - h, halves[h], :] + rx[0, i, h]
            start(
                fw.at[i, h], rx.at[2, i, h], x_send.at[0], x_recv.at[i],
                device(near[1 - h], y, core, par),
            )

    def own(i):
        px[i] = partial_for(ks[i], x)

    def finish(i):
        await_bytes(ry, x_recv.at[i])
        total = px[i] + (rx[1, i] + rx[2, i]).reshape(HD, HD)
        ys[i] = total.T
        farther = {0: 0, 1: 1, 2: mine, 3: 0}[order[i]]
        for j in (farther, 1 - farther):
            rows = pl.ds(pl.multiple_of(j * HALF, HALF), HALF)
            start(
                ys.at[i, rows], yr.at[y], y_send.at[0], y_recv.at[0],
                device(x, 2 * ks[i] + j, core, par),
            )

    beside = 2 * ky + 1 - mine
    last = chunks - 1

    def compute_pair():
        await_bytes(fr.at[ks[last]], f_recv.at[last])
        for m in range(2):
            sy[m] = partial_pair(ks[last], xs[m], 1 - mine, xs[m + 2], 1 - mine)

    def send_pair():
        for m in range(2):
            start(sy.at[m], ry.at[m], p_send.at[0], p_recv.at[m], device(x, beside, core, par))

    def keep_pair():
        for m in range(2):
            sk[m] = partial_pair(ks[last], xs[m], mine, xs[m + 2], mine)

    def spread_pair():
        for m in (0, 1):
            await_bytes(ry.at[m], p_recv.at[m])
            qs[m] = (sk[m] + ry[m]).T
            for d in ((2,), (1, 3))[m]:
                start(
                    qs.at[m, halves[d // 2]], xd.at[d - 1], d_send.at[0], d_recv.at[0],
                    device(xs[d], y, core, par),
                )

    main = range(last)
    compute_far(0)
    send_far(0)
    compute_near(0)
    send_near(0)
    for i in main[1:]:
        compute_far(i)
    for i in main[1:]:
        send_far(i)
    compute_pair()
    send_pair()
    step_two(0)
    for i in main[1:]:
        compute_near(i)
        send_near(i)
    for i in main[1:]:
        step_two(i)
    keep_pair()
    own(0)
    finish(0)
    spread_pair()
    for i in main[1:]:
        own(i)
    for i in main[1:]:
        finish(i)

    mom_load.wait()
    grads = qs[0, halves[0], :]
    await_bytes(xd, d_recv.at[0])
    for d in (1, 2, 3):
        grads = grads + xd[d - 1]
    await_bytes(yr.at[pl.ds(0, ny - 2)], y_recv.at[0])
    for i in main:
        for j in range(2):
            grads = grads + yr[2 * ks[i] + j]

    grads_out[...] = grads
    blend = grads + retain * (retain * mv[...] + grads)
    contract = (((0,), (0,)), ((), ()))
    gs[...] = lax.dot_general(
        blend, blend, contract, precision=PRECISE, preferred_element_type=jnp.float32
    ).reshape(8, 16, HD)

    owner = x * 2 + par
    owners = [(xs[dx], ps[dp]) for dx in (2, 1, 3, 0) for dp in (1, 0)]
    for xx, pp in owners[:-1]:
        start(
            gs.at[xx * 2 + pp], gr.at[member], g_send.at[0], g_recv.at[0], device(xx, y, 1, pp)
        )

    @pl.when(core == 0)
    def _():
        start(gs.at[owner], gr.at[member], g_send.at[0], g_recv.at[0], device(x, y, 1, par))
        await_bytes(ag, g_recv.at[2])

    @pl.when(core == 1)
    def _():
        gr[member] = gs[owner]
        await_bytes(gr.at[pl.ds(0, 15)], g_recv.at[0])
        hr[y] = jnp.sum(gr[...], axis=0)
        for d in far_first:
            start(hr.at[y], hr.at[y], g_send.at[1], g_recv.at[1], device(x, yy[d], 1, par))
        await_bytes(hr.at[pl.ds(0, ny - 1)], g_recv.at[1])
        ag[owner] = jnp.sum(hr[...], axis=0)
        for xx, cc, pp in others:
            start(ag.at[owner], ag.at[owner], g_send.at[2], g_recv.at[2], device(xx, y, cc, pp))
        await_bytes(ag.at[pl.ds(0, 7)], g_recv.at[2])

    gram = ag[...].reshape(HD, HD)
    row = lax.broadcasted_iota(jnp.int32, (HD, HD), 0)
    identity = jnp.where(row == lane, 1.0, 0.0).astype(jnp.float32)
    total = jnp.sum(gram * identity, axis=(0, 1), keepdims=True)
    inverse = 1.0 / (jnp.sqrt(total) + epsilon)

    def parts(a):
        first_part = a.astype(jnp.bfloat16)
        rest = a - first_part.astype(jnp.float32)
        second_part = rest.astype(jnp.bfloat16)
        third_part = (rest - second_part.astype(jnp.float32)).astype(jnp.bfloat16)
        return first_part, second_part, third_part

    def dot(a, b):
        a1, a2, a3 = a
        b1, b2, b3 = b
        m = a1.shape[0]
        upper = jnp.concatenate([a1, a2], axis=0)
        high = jnp.dot(
            jnp.concatenate([upper, upper], axis=1),
            jnp.concatenate([b1, b2], axis=0),
            preferred_element_type=jnp.float32,
        )
        low = jnp.dot(
            jnp.concatenate([a1, a3], axis=1),
            jnp.concatenate([b3, b1], axis=0),
            preferred_element_type=jnp.float32,
        )
        return high[:m] + (high[m:] + low)

    state = blend * inverse
    gram = gram * (inverse * inverse)
    for step in range(ITERS):
        split = parts(gram)
        square = dot(split, split)
        poly = parts(first_coef * identity + second_coef * gram + third_coef * square)
        if step < ITERS - 1:
            both = [
                jnp.concatenate([g, t], axis=0) for g, t in zip(split, parts(state))
            ]
            both = dot(both, poly)
            state = both[HD:]
            gram = dot(parts(both[:HD]), poly)
        else:
            state = dot(parts(state), poly)
    state_out[...] = state

    await_bytes(kv.at[pl.ds(1, 3)], key_sem.at[0])
    await_bytes(fr, f_send.at[0])
    await_bytes(rx, x_send.at[0])
    await_bytes(yr.at[pl.ds(0, ny - 2)], y_send.at[0])
    await_bytes(ry, p_send.at[0])
    await_bytes(xd, d_send.at[0])
    await_bytes(gs.at[pl.ds(0, 7)], g_send.at[0])

    @pl.when(core == 0)
    def _():
        await_bytes(gs.at[0], g_send.at[0])

    @pl.when(core == 1)
    def _():
        await_bytes(hr.at[pl.ds(0, ny - 1)], g_send.at[1])
        await_bytes(gr.at[pl.ds(0, 15)], g_send.at[2])


def on_device(features, key_partials, momentum):
    ny = lax.axis_size("fsdp") // (2 * NX)
    chunks = ny // 2
    main = chunks - 1
    f32, bf16 = jnp.float32, jnp.bfloat16
    dma = pltpu.SemaphoreType.DMA
    block = jax.ShapeDtypeStruct((HALF, HD), f32)
    hbm = pl.BlockSpec(memory_space=pltpu.HBM)
    vmem = pl.BlockSpec(memory_space=pltpu.VMEM)
    moment = momentum[:, 0, :]

    def body(*refs):
        step_kernel(ny, *refs)

    state, grads = pl.pallas_call(
        body,
        name="muon_step",
        out_shape=(block, block),
        in_specs=[hbm] * 3,
        out_specs=(vmem, vmem),
        scratch_shapes=[
            pltpu.VMEM((chunks, NX, HD, 4 * HD), bf16),
            pltpu.VMEM((chunks, NX, HD, 2 * HD), bf16),
            pltpu.VMEM((4, HD, HD), bf16),
            pltpu.VMEM((2 * HD, 2 * HD), bf16),
            pltpu.VMEM((HALF, HD), f32),
            pltpu.VMEM((main, HD, HD), f32),
            pltpu.VMEM((main, 2, HD, HD), f32),
            pltpu.VMEM((main, HD, HD), f32),
            pltpu.VMEM((3, main, 2, HALF, HD), f32),
            pltpu.VMEM((main, 2, HALF, HD), f32),
            pltpu.VMEM((main, HD, HD), f32),
            pltpu.VMEM((ny, HALF, HD), f32),
            pltpu.VMEM((2, HD, HD), f32),
            pltpu.VMEM((2, HD, HD), f32),
            pltpu.VMEM((2, HD, HD), f32),
            pltpu.VMEM((2, HD, HD), f32),
            pltpu.VMEM((NX - 1, HALF, HD), f32),
            pltpu.VMEM((8, 16, HD), f32),
            pltpu.VMEM((16, 16, HD), f32),
            pltpu.VMEM((ny, 16, HD), f32),
            pltpu.VMEM((8, 16, HD), f32),
            dma((chunks + 2,)),
            dma((3,)),
            dma((1,)), dma((chunks,)),
            dma((1,)), dma((main,)), dma((main, 2)),
            dma((1,)), dma((1,)),
            dma((1,)), dma((2,)),
            dma((1,)), dma((1,)),
            dma((3,)), dma((3,)),
        ],
        compiler_params=pltpu.CompilerParams(
            collective_id=0, has_side_effects=True, vmem_limit_bytes=16 * 1024 * 1024
        ),
    )(*(pltpu.with_memory_space_constraint(v, pltpu.HBM) for v in (features, key_partials[:, 0, :], moment)))
    update = shrink * math.sqrt(D_W) * state
    return (update[:, None, :], (retain * moment + grads)[:, None, :])


def solution(mesh):
    placed = (P("fsdp", None), P("fsdp", "tp", None), P("fsdp", "tp", None))
    return jax.shard_map(
        on_device,
        mesh=mesh,
        in_specs=placed,
        out_specs=(P("fsdp", "tp", None), P("fsdp", "tp", None)),
        check_vma=False,
    )
```
